256 devices in a mesh: fsdp: 32 (over z, y), rep: 8 (over x, core).
Axes of the slice: x: 4, y: 4, z: 8, core: 2. Of those that a mesh axis runs over, the one named last changes fastest.
Arguments:
- hidden: bfloat16 [65536, 2048], P(('fsdp', 'rep')), may hold values from -6 to 6
- attn_gain: bfloat16 [2048], P(('fsdp', 'rep')), may hold values from 0.25 to 1.75
- w_query: bfloat16 [2048, 2048], P(('fsdp', 'rep')), as said below
- w_key: bfloat16 [2048, 512], P(('fsdp', 'rep')), as said below
- w_value: bfloat16 [2048, 512], P(('fsdp', 'rep')), may hold values from -0.125 to 0.125
- w_out: bfloat16 [2048, 2048], P(None, ('fsdp', 'rep')), may hold values from -0.125 to 0.125
Outputs:
- mixed: bfloat16 [65536, 2048], P(('fsdp', 'rep'))
The draws below stay inside these ranges and needn't reach their ends.
Inputs may be any that keep to these rules, and one draw needn't show every extreme that they name: `w_query`: entries of order 2048^(-1/2). `w_key`: entries of order 2048^(-1/2) times a factor up to twenty.
All inputs are finite; a program needn't handle non-finite values.
Results may differ from the reference program's by a relative error of at most 0.012.
The reference program's roundings to bfloat16 on the way (of `normed`, `probs` and `context`) count: a program that leaves them out, or rounds other values in their place, can miss the bound.
Values may be sent and summed in bfloat16 or wider, within the bound.
No kernel may reach another device: no remote copies, remote signals or barrier semaphores. Data moves between devices by JAX's collectives and lax.ppermute only.
A program may use at most 64 MiB of HBM per device.

```python
import math
import jax
import jax.numpy as jnp
from jax import lax

D = 2048
HEADS = 32
KV_HEADS = 8
HD = 64
TOK_DEV = 256
TOKENS = 65536
N_FSDP = 32
N_REP = 8


def shared_base(key):
    return jax.random.normal(jax.random.fold_in(key, 7), (D, KV_HEADS, 1, HD), jnp.float32) / math.sqrt(D)


def draw_w_query(key, part):
    group = HEADS // KV_HEADS
    others = jax.random.normal(jax.random.fold_in(key, 11), (D, KV_HEADS, group, HD), jnp.float32) / math.sqrt(D)
    joined = jnp.concatenate([shared_base(key), others[:, :, 1:, :]], axis=2)
    return joined.reshape(D, HEADS * HD).astype(jnp.bfloat16)


def draw_w_key(key, part):
    noise = jax.random.normal(jax.random.fold_in(key, 13), (D, KV_HEADS * HD), jnp.float32) / math.sqrt(D)
    result = noise
    return result.astype(jnp.bfloat16)


def block_levels(stream_key, extent, shards, least, high):
    def one(dim, parts):
        draws = jax.random.uniform(jax.random.fold_in(jax.random.fold_in(stream_key, 6), dim), (parts,), jnp.float32, least / len(shards), high / len(shards))
        return jnp.repeat(jnp.exp(draws), extent[dim] // parts).reshape((-1,) + (1,) * (len(extent) - dim - 1))

    level = one(*shards[0])
    for cut in shards[1:]:
        level = level * one(*cut)
    return level


def normal_values(key, extent, spread, most, split=(), held_as=jnp.bfloat16):
    values = jax.random.normal(key, extent, jnp.float32) * spread
    if len(split) > 0:
        values = block_levels(key, extent, split, -0.22, 0.18) * values
    return jnp.clip(values, min=-most, max=most).astype(held_as)


def setup_inputs(seed: int = 0) -> dict:
    streams_of = jax.random.split(jax.random.key(seed), 7)
    return {
        "hidden": normal_values(streams_of[0], (TOKENS, D), 1.0, 6.0, ((0, 256),)),
        "attn_gain": jnp.clip(1.0 + 0.15 * jax.random.normal(streams_of[1], (D,), jnp.float32), 0.25, 1.75).astype(jnp.bfloat16),
        "w_query": draw_w_query(jax.random.fold_in(streams_of[6], 71), 0),
        "w_key": draw_w_key(jax.random.fold_in(streams_of[6], 71), 0),
        "w_value": normal_values(streams_of[4], (D, KV_HEADS * HD), D ** -0.5, 0.125, ((0, 256),)),
        "w_out": normal_values(streams_of[5], (HEADS * HD, D), (HEADS * HD) ** -0.5, 0.125, ((1, 256),)),
    }


rope_base = 500000.0
norm_eps = 1e-05

def rope_tables(tokens, head_dim):
    position = jnp.arange(tokens, dtype=jnp.float32)
    freq = rope_base ** (-(jnp.arange(head_dim // 2, dtype=jnp.float32) * 2.0) / head_dim)
    angle = position[:, None] * freq[None, :]
    cos_table = jnp.concatenate([jnp.cos(angle), jnp.cos(angle)], axis=-1)
    sin_table = jnp.concatenate([jnp.sin(angle), jnp.sin(angle)], axis=-1)
    return (cos_table, sin_table)

def rotate(tensor, cos_table, sin_table):
    half = tensor.shape[-1] // 2
    turned = jnp.concatenate([-tensor[..., half:], tensor[..., :half]], axis=-1)
    return tensor * cos_table + turned * sin_table

def reference(hidden, attn_gain, w_query, w_key, w_value, w_out):
    group = HEADS // KV_HEADS
    cos_table, sin_table = rope_tables(TOK_DEV, HD)
    causal = jnp.arange(TOK_DEV)[:, None] >= jnp.arange(TOK_DEV)[None, :]

    def one_sequence(block):
        x_float = block.astype(jnp.float32)
        inv_rms = lax.rsqrt(lax.optimization_barrier(jnp.mean(x_float * x_float, axis=-1, keepdims=True)) + norm_eps)
        normed = (x_float * inv_rms * attn_gain.astype(jnp.float32)[None, :]).astype(jnp.bfloat16)
        queries = jnp.dot(normed, w_query, preferred_element_type=jnp.float32)
        keys_raw = jnp.dot(normed, w_key, preferred_element_type=jnp.float32)
        values_raw = jnp.dot(normed, w_value, preferred_element_type=jnp.float32)
        queries = queries.reshape(TOK_DEV, KV_HEADS, group, HD)
        keys_raw = keys_raw.reshape(TOK_DEV, KV_HEADS, HD)
        values_bf = values_raw.reshape(TOK_DEV, KV_HEADS, HD).astype(jnp.bfloat16)
        rope_queries = rotate(queries, cos_table[:, None, None, :], sin_table[:, None, None, :]).astype(jnp.bfloat16)
        rope_keys = rotate(keys_raw, cos_table[:, None, :], sin_table[:, None, :]).astype(jnp.bfloat16)
        scores = jnp.einsum('qkgd,skd->kgqs', rope_queries.astype(jnp.float32), rope_keys.astype(jnp.float32)) * HD ** (-0.5)
        scores = jnp.where(causal[None, None, :, :], scores, -1e+30)
        top = lax.optimization_barrier(jnp.max(scores, axis=-1, keepdims=True))
        expo = jnp.exp(scores - top)
        probs = (expo / lax.optimization_barrier(jnp.sum(expo, axis=-1, keepdims=True))).astype(jnp.bfloat16)
        context = jnp.einsum('kgqs,skd->qkgd', probs.astype(jnp.float32), values_bf.astype(jnp.float32))
        context = context.reshape(TOK_DEV, HEADS * HD).astype(jnp.bfloat16)
        return (x_float + jnp.dot(context, w_out, preferred_element_type=jnp.float32)).astype(jnp.bfloat16)
    blocks = hidden.reshape(N_FSDP * N_REP, TOK_DEV, D)
    return lax.map(one_sequence, blocks).reshape(TOKENS, D)
```

```python
import jax
import jax.numpy as jnp
from jax import lax
from jax.sharding import PartitionSpec as P

HD = 64
PAD = 128

rope_base = 500000.0
norm_eps = 1e-05


def rope_tables(tokens, head_dim):
    position = jnp.arange(tokens, dtype=jnp.float32)
    freq = rope_base ** (-(jnp.arange(head_dim // 2, dtype=jnp.float32) * 2.0) / head_dim)
    angle = position[:, None] * freq[None, :]
    cos_table = jnp.concatenate([jnp.cos(angle), jnp.cos(angle)], axis=-1)
    sin_table = jnp.concatenate([jnp.sin(angle), jnp.sin(angle)], axis=-1)
    return (cos_table, sin_table)


def rotate(tensor, cos_table, sin_table):
    half = tensor.shape[-1] // 2
    turned = jnp.concatenate([-tensor[..., half:], tensor[..., :half]], axis=-1)
    return tensor * cos_table + turned * sin_table


def body(hidden, attn_gain, w_query, w_key, w_value, w_out):
    tokens = hidden.shape[0]
    head_dim = HD
    width_query = w_query.shape[1]
    width_kv = w_key.shape[1]
    kv_count = width_kv // head_dim
    group = width_query // width_kv
    x_float = hidden.astype(jnp.float32)
    inv_rms = lax.rsqrt(jnp.mean(x_float * x_float, axis=-1, keepdims=True) + norm_eps)
    gain_column = jnp.broadcast_to(attn_gain[:, None], (attn_gain.shape[0], PAD))
    rows = jnp.concatenate([w_query, w_key, w_value, w_out.T, gain_column], axis=1)
    every = lax.all_gather(rows, ("fsdp", "rep"), axis=0, tiled=True)
    at = 0
    pieces = []
    for width in (width_query, width_kv, width_kv, w_out.shape[0]):
        pieces.append(every[:, at : at + width])
        at += width
    query_piece, key_piece, value_piece, out_piece = pieces
    gain_piece = every[:, at]
    normed = (x_float * inv_rms * gain_piece.astype(jnp.float32)[None, :]).astype(jnp.bfloat16)
    queries = jnp.dot(normed, query_piece, preferred_element_type=jnp.float32)
    keys_raw = jnp.dot(normed, key_piece, preferred_element_type=jnp.float32)
    values_raw = jnp.dot(normed, value_piece, preferred_element_type=jnp.float32)
    cos_table, sin_table = rope_tables(tokens, head_dim)
    queries = queries.reshape(tokens, kv_count, group, head_dim)
    keys_raw = keys_raw.reshape(tokens, kv_count, head_dim)
    values_bf = values_raw.reshape(tokens, kv_count, head_dim).astype(jnp.bfloat16)
    rope_queries = rotate(queries, cos_table[:, None, None, :], sin_table[:, None, None, :]).astype(
        jnp.bfloat16
    )
    rope_keys = rotate(keys_raw, cos_table[:, None, :], sin_table[:, None, :]).astype(jnp.bfloat16)
    scores = jnp.einsum(
        "qkgd,skd->kgqs", rope_queries, rope_keys, preferred_element_type=jnp.float32
    ) * head_dim ** (-0.5)
    causal = jnp.arange(tokens)[:, None] >= jnp.arange(tokens)[None, :]
    scores = jnp.where(causal[None, None, :, :], scores, -1e30)
    top = jnp.max(scores, axis=-1, keepdims=True)
    expo = jnp.exp(scores - top)
    probs = (expo / jnp.sum(expo, axis=-1, keepdims=True)).astype(jnp.bfloat16)
    context = jnp.einsum("kgqs,skd->qkgd", probs, values_bf, preferred_element_type=jnp.float32)
    context = context.reshape(tokens, width_query).astype(jnp.bfloat16)
    branch = lax.dot_general(
        context, out_piece, (((1,), (1,)), ((), ())), preferred_element_type=jnp.float32
    )
    return (x_float + branch).astype(jnp.bfloat16)


def solution(mesh):
    placed = (
        P(("fsdp", "rep"), None),
        P(("fsdp", "rep")),
        P(("fsdp", "rep"), None),
        P(("fsdp", "rep"), None),
        P(("fsdp", "rep"), None),
        P(None, ("fsdp", "rep")),
    )
    return jax.shard_map(
        body, mesh=mesh, in_specs=placed, out_specs=P(("fsdp", "rep"), None), check_vma=False
    )
```

```python
import functools

import jax
import jax.numpy as jnp
from jax import lax
from jax.experimental import pallas as pl
from jax.experimental.pallas import tpu as pltpu
from jax.sharding import Mesh
from jax.sharding import PartitionSpec as P


HD = 64
PAD = 128
AXES = ("z", "y", "x", "c")
VMEM = pl.BlockSpec(memory_space=pltpu.VMEM)
SMEM = pl.BlockSpec(memory_space=pltpu.SMEM)
ANY = pl.BlockSpec(memory_space=pl.ANY)
F32 = jnp.float32
BF16 = jnp.bfloat16

rope_base = 500000.0
norm_eps = 1e-05


def shape_of(dims, dtype=BF16):
    return jax.ShapeDtypeStruct(tuple(dims), dtype)


def shift(array, axis, by):
    n = lax.axis_size(axis)
    return lax.ppermute(array, axis, [(i, (i + by) % n) for i in range(n)])


def halves_kernel(at, wq, wk, wv, gain, wo, mine, theirs):
    core = at[0]
    for out, which in ((mine, core), (theirs, 1 - core)):
        to = 0
        for ref, dtype_cols in ((wk, 2), (wv, 2), (gain, 1), (wq, 2), (wo, 2)):
            n = ref.shape[1] // dtype_cols
            start = 0 if dtype_cols == 1 else pl.multiple_of(which * n, 128)
            out[:, to : to + n] = ref[:, pl.ds(start, n)]
            to += n


def order_kernel(cols, at, mine, got, copies, outs):
    core = at[0]
    rows = mine.shape[0]
    for k in range(2):
        piece = jnp.where(core == k, mine[...], got[...])
        for z in range(copies.shape[0]):
            copies[z, k * rows : (k + 1) * rows, :] = piece[:, :cols]
        outs[k * rows : (k + 1) * rows, :] = piece[:, cols:]


def beside_kernel(dim, n, slot, at, *refs):
    *pieces, out = refs
    me = at[slot]
    for by, ref in zip((0, n - 1, 1, 2, 2), pieces):
        index = lax.rem(me + by, n)
        if dim == 0:
            out[index] = ref[...]
        elif ref.shape[0] == out.shape[0]:
            out[:, pl.ds(index, 1)] = ref[...][:, None]
    if dim == 1:
        low, high = pieces[3], pieces[4]
        half = low.shape[0]
        index = lax.rem(me + 2, n)
        out[0:half, pl.ds(index, 1)] = low[...][:, None]
        out[half : 2 * half, pl.ds(index, 1)] = high[...][:, None]


def beside(at, slot, pieces, dim):
    dims = list(pieces[0].shape)
    dims.insert(dim, 4)
    return pl.pallas_call(
        functools.partial(beside_kernel, dim, 4, slot),
        out_shape=shape_of(dims),
        in_specs=[SMEM] + [VMEM] * len(pieces),
        out_specs=VMEM,
        name="beside",
    )(at, *pieces)


def ring4(block, axis):
    half = block.shape[0] // 2
    back = shift(block, axis, 1)
    ahead = shift(block, axis, -1)
    low = shift(back[:half], axis, 1)
    high = shift(ahead[half:], axis, -1)
    return block, back, ahead, low, high


def direct4(at, slot, block, axis):
    back = shift(block, axis, 1)
    ahead = shift(block, axis, -1)
    far = shift(block, axis, 2)
    return beside(at, slot, (block, back, ahead, far), 0)


def ring8(block, axis):
    half = block.shape[0] // 2
    back = ahead = block
    pieces = [block]
    for _ in range(3):
        back = shift(back, axis, 1)
        ahead = shift(ahead, axis, -1)
        pieces += [back, ahead]
    return (*pieces, shift(back[:half], axis, 1), shift(ahead[half:], axis, -1))


def attend_kernel(tokens, at, own, other, cos_ref, sin_ref, *refs):
    a_pieces, b_pieces = refs[0:5], refs[5:10]
    ctx, w_a, w_b, normed, q_s, k_s, v_s, sems = refs[10:]
    width = own.shape[1]
    x_at, y_at = at[1], at[2]
    copies = []
    for i, (by, z0, zn) in enumerate(((0, 0, 8), (3, 0, 8), (1, 0, 8), (2, 0, 4), (2, 4, 4))):
        y_from = lax.rem(y_at + by, 4)
        x_from = lax.rem(x_at + by, 4)
        copies.append(pltpu.make_async_copy(a_pieces[i], w_a.at[pl.ds(z0, zn), y_from], sems.at[i]))
        copies.append(
            pltpu.make_async_copy(b_pieces[i], w_b.at[pl.ds(z0, zn), :, x_from], sems.at[5 + i])
        )
    for c in copies:
        c.start()
    kv_cols = k_s.shape[1]
    for c in copies:
        c.wait()
    gain = w_a[:, :, :, :, 2 * kv_cols : 2 * kv_cols + PAD].reshape(width // PAD, PAD, PAD).astype(F32)
    eye = lax.broadcasted_iota(jnp.int32, (PAD, PAD), 0) == lax.broadcasted_iota(jnp.int32, (PAD, PAD), 1)
    lanes = jnp.concatenate(
        [jnp.sum(jnp.where(eye, gain[i], 0.0), axis=0, keepdims=True) for i in range(width // PAD)], axis=1
    )
    step = 64

    def norm(i, _):
        for s, ref in enumerate((own, other)):
            start = pl.multiple_of(i * step, step)
            x = ref[pl.ds(start, step), :].astype(F32)
            inv = lax.rsqrt(jnp.sum(x * x, axis=1, keepdims=True) * (1.0 / width) + norm_eps)
            normed[pl.ds(s * tokens + start, step), :] = (x * inv * lanes).astype(BF16)
        return 0

    lax.fori_loop(0, tokens // step, norm, 0)

    low_half = (lax.broadcasted_iota(jnp.int32, (tokens, 2 * HD), 1) % HD) < HD // 2

    def rope(t):
        turned = jnp.where(low_half, -pltpu.roll(t, 2 * HD - HD // 2, 1), pltpu.roll(t, HD // 2, 1))
        return t * cos_ref[...] + turned * sin_ref[...]

    def product(s, weights):
        start = pl.multiple_of(s * tokens, tokens)
        return jnp.dot(normed[pl.ds(start, tokens), :], weights, preferred_element_type=F32)

    def keys_values(s, _):
        start = pl.multiple_of(s * tokens, tokens)
        t = product(s, w_a[:, :, :, :, 0:kv_cols].reshape(width, kv_cols))
        for j in range(kv_cols // (2 * HD)):
            cols = slice(j * 2 * HD, (j + 1) * 2 * HD)
            k_s[pl.ds(start, tokens), cols] = rope(t[:, cols]).astype(BF16)
        t = product(s, w_a[:, :, :, :, kv_cols : 2 * kv_cols].reshape(width, kv_cols))
        v_s[s] = t.T.astype(BF16)
        return 0

    lax.fori_loop(0, 2, keys_values, 0)

    def queries(s, _):
        start = pl.multiple_of(s * tokens, tokens)
        base = 2 * kv_cols + PAD
        for n in range(4):
            if n == 0:
                weights = w_a[:, :, :, :, base : base + kv_cols]
            else:
                weights = w_b[:, :, :, :, (n - 1) * kv_cols : n * kv_cols]
            t = product(s, weights.reshape(width, kv_cols))
            for j in range(kv_cols // (2 * HD)):
                cols = slice(j * 2 * HD, (j + 1) * 2 * HD)
                to = n * kv_cols + j * 2 * HD
                q_s[pl.ds(start, tokens), to : to + 2 * HD] = rope(t[:, cols]).astype(BF16)
        return 0

    lax.fori_loop(0, 2, queries, 0)

    seen = lax.broadcasted_iota(jnp.int32, (tokens, tokens), 0) <= lax.broadcasted_iota(
        jnp.int32, (tokens, tokens), 1
    )
    left = lax.broadcasted_iota(jnp.int32, (tokens, 2 * HD), 1) < HD

    def attend(s, _):
        start = pl.multiple_of(s * tokens, tokens)
        for kv in range(4):
            tile = k_s[pl.ds(start, tokens), (kv // 2) * 2 * HD : (kv // 2 + 1) * 2 * HD].astype(F32)
            in_left = jnp.where(left, tile if kv % 2 == 0 else pltpu.roll(tile, HD, 1), 0.0)
            sides = (in_left.astype(BF16), pltpu.roll(in_left, HD, 1).astype(BF16))
            parts = []
            for g in range(4):
                h = kv * 4 + g
                q = q_s[pl.ds(start, tokens), (h // 2) * 2 * HD : (h // 2 + 1) * 2 * HD]
                scores = lax.dot_general(
                    sides[h % 2], q, (((1,), (1,)), ((), ())), preferred_element_type=F32
                )
                scores = jnp.where(seen, scores * HD**-0.5, -1e30)
                expo = jnp.exp(scores - jnp.max(scores, axis=0, keepdims=True))
                probs = (expo * (1.0 / jnp.sum(expo, axis=0, keepdims=True))).astype(BF16)
                parts.append(
                    jnp.dot(v_s[s, kv * HD : (kv + 1) * HD, :], probs, preferred_element_type=F32)
                )
            ctx[pl.ds(start, tokens), kv * 4 * HD : (kv + 1) * 4 * HD] = (
                jnp.concatenate(parts, axis=0).T.astype(BF16)
            )
        return 0

    lax.fori_loop(0, 2, attend, 0)


def project_kernel(seq, tokens, at, ctx, *refs):
    pieces = refs[0:9]
    out, w_o, sems = refs[9:]
    z_at = at[3]
    rows = w_o.shape[1]
    half = rows // 2
    copies = []
    for i, by in enumerate((0, 7, 1, 6, 2, 5, 3, 4, 4)):
        z_from = lax.rem(z_at + by, 8)
        to = w_o.at[z_from]
        if i == 7:
            to = w_o.at[z_from, 0:half]
        if i == 8:
            to = w_o.at[z_from, half:rows]
        copies.append(pltpu.make_async_copy(pieces[i], to, sems.at[i]))
    for c in copies:
        c.start()
    for c in copies:
        c.wait()

    def one(z, _):
        out[:, pl.ds(pl.multiple_of(z * rows, rows), rows)] = lax.dot_general(
            ctx[seq * tokens : (seq + 1) * tokens, :],
            w_o[z],
            (((1,), (1,)), ((), ())),
            preferred_element_type=F32,
        )
        return 0

    lax.fori_loop(0, 8, one, 0)


def inner(hidden, attn_gain, w_query, w_key, w_value, w_out):
    tokens, width = hidden.shape
    wq, wkv = w_query.shape[1] // 2, w_key.shape[1] // 2
    rows = w_query.shape[0]
    cols = wq + 2 * wkv + PAD
    cols_a = 3 * wkv + PAD
    at = jnp.stack([lax.axis_index(a) for a in ("c", "x", "y", "z")]).astype(jnp.int32)

    gain = jnp.broadcast_to(attn_gain[:, None], (rows, PAD))
    mine, theirs = pl.pallas_call(
        halves_kernel,
        out_shape=(shape_of((rows, cols + wq)),) * 2,
        in_specs=[SMEM] + [VMEM] * 5,
        out_specs=(VMEM, VMEM),
        name="halves",
    )(at, w_query, w_key, w_value, gain, w_out.T)
    got = shift(theirs, "c", 1)
    copies, out_rows = pl.pallas_call(
        functools.partial(order_kernel, cols),
        out_shape=(shape_of((8, 2 * rows, cols)), shape_of((2 * rows, wq))),
        in_specs=[SMEM, VMEM, VMEM],
        out_specs=(VMEM, VMEM),
        name="order",
    )(at, mine, got)
    by_z = lax.all_to_all(copies, "z", split_axis=0, concat_axis=0, tiled=True)
    other = shift(hidden, "c", 1)
    out_x = direct4(at, 1, out_rows, "x")
    out_xy = direct4(at, 2, out_x, "y").reshape(-1, wq)
    out_pieces = ring8(out_xy, "z")
    block_a = beside(at, 1, ring4(by_z[:, :, :cols_a], "x"), 1)
    block_b = beside(at, 2, ring4(by_z[:, :, cols_a:], "y"), 1)
    a_pieces = ring4(block_a, "y")
    b_pieces = ring4(block_b, "x")

    position = jnp.arange(tokens, dtype=F32)
    freq = rope_base ** (-(jnp.arange(HD // 2, dtype=F32) * 2.0) / HD)
    angle = position[:, None] * freq[None, :]
    cos_table = jnp.concatenate([jnp.cos(angle)] * 4, axis=-1)
    sin_table = jnp.concatenate([jnp.sin(angle)] * 4, axis=-1)

    context = pl.pallas_call(
        functools.partial(attend_kernel, tokens),
        out_shape=shape_of((2 * tokens, wq)),
        in_specs=[SMEM] + [VMEM] * 4 + [ANY] * 10,
        out_specs=VMEM,
        scratch_shapes=[
            pltpu.VMEM((8, 4, 4, 2 * rows, cols_a), BF16),
            pltpu.VMEM((8, 4, 4, 2 * rows, cols - cols_a), BF16),
            pltpu.VMEM((2 * tokens, width), BF16),
            pltpu.VMEM((2 * tokens, wq), BF16),
            pltpu.VMEM((2 * tokens, wkv), BF16),
            pltpu.VMEM((2, wkv, tokens), BF16),
            pltpu.SemaphoreType.DMA((10,)),
        ],
        cost_estimate=pl.CostEstimate(flops=4_000_000_000, bytes_accessed=10_000_000, transcendentals=0),
        compiler_params=pltpu.CompilerParams(vmem_limit_bytes=40 * 1024 * 1024),
        name="attend",
    )(at, hidden, other, cos_table, sin_table, *a_pieces, *b_pieces)

    def project(seq):
        return pl.pallas_call(
            functools.partial(project_kernel, seq, tokens),
            out_shape=shape_of((tokens, width), F32),
            in_specs=[SMEM, VMEM] + [ANY] * 9,
            out_specs=VMEM,
            scratch_shapes=[pltpu.VMEM((8, width // 8, wq), BF16), pltpu.SemaphoreType.DMA((9,))],
            cost_estimate=pl.CostEstimate(flops=1_000_000_000, bytes_accessed=8_000_000, transcendentals=0),
            compiler_params=pltpu.CompilerParams(vmem_limit_bytes=24 * 1024 * 1024),
            name="project",
        )(at, context, *out_pieces)

    from_them = shift(project(1), "c", 1)
    return (hidden.astype(F32) + (project(0) + from_them)).astype(BF16)


def solution(mesh):
    torus = Mesh(mesh.devices.reshape(8, 4, 4, 2), AXES)
    placed = (P(AXES, None), P(AXES), P(AXES, None), P(AXES, None), P(AXES, None), P(None, AXES))
    return jax.shard_map(inner, mesh=torus, in_specs=placed, out_specs=P(AXES, None), check_vma=False)
```

```python
import functools

import jax
import jax.numpy as jnp
from jax import lax
from jax.experimental import pallas as pl
from jax.experimental.pallas import tpu as pltpu
from jax.sharding import Mesh
from jax.sharding import PartitionSpec as P


HD = 64
PAD = 128
AXES = ("z", "y", "x", "c")
VMEM = pl.BlockSpec(memory_space=pltpu.VMEM)
SMEM = pl.BlockSpec(memory_space=pltpu.SMEM)
ANY = pl.BlockSpec(memory_space=pl.ANY)
F32 = jnp.float32
BF16 = jnp.bfloat16

rope_base = 500000.0
norm_eps = 1e-05


def shape_of(dims, dtype=BF16):
    return jax.ShapeDtypeStruct(tuple(dims), dtype)


def shift(array, axis, by):
    n = lax.axis_size(axis)
    return lax.ppermute(array, axis, [(i, (i + by) % n) for i in range(n)])


def halves_kernel(at, gain, wk, wv, wq, wo, copies, mine, theirs):
    core = at[0]
    rows = wq.shape[0]
    eye = lax.broadcasted_iota(jnp.int32, (rows, rows), 0) == lax.broadcasted_iota(jnp.int32, (rows, rows), 1)
    column = jnp.sum(jnp.where(eye, gain[...].astype(F32), 0.0), axis=1, keepdims=True)
    wide = jnp.broadcast_to(column, (rows, PAD)).astype(BF16)
    for which in range(2):
        pieces = []
        for ref in (wk, wv, wq):
            n = ref.shape[1] // 2
            pieces.append(ref[:, which * n : (which + 1) * n])
        row = jnp.concatenate(pieces[:2] + [wide] + pieces[2:], axis=1)
        for z in range(copies.shape[0] // 2):
            copies[2 * z + which] = row
    n = wo.shape[1] // 2
    mine[...] = wo[:, pl.ds(pl.multiple_of(core * n, 128), n)]
    theirs[...] = wo[:, pl.ds(pl.multiple_of((1 - core) * n, 128), n)]


def order_kernel(at, mine, got, out):
    rows = mine.shape[0]
    for k in range(2):
        out[k * rows : (k + 1) * rows, :] = jnp.where(at[0] == k, mine[...], got[...])


def split_kernel(by_z, a, b):
    n, m = a.shape[3], b.shape[2]
    for k in range(a.shape[0]):
        a[k] = by_z[:, :, 0:n]
    b[...] = by_z[:, :, n : n + m]


def to_all(array, axes):
    return lax.all_to_all(array, axes, split_axis=0, concat_axis=0, tiled=True)


def beside_kernel(dim, n, slot, at, *refs):
    *pieces, out = refs
    me = at[slot]
    for by, ref in zip((0, n - 1, 1, 2, 2), pieces):
        index = lax.rem(me + by, n)
        if dim == 0:
            out[index] = ref[...]
        elif ref.shape[0] == out.shape[0]:
            out[:, pl.ds(index, 1)] = ref[...][:, None]
    if dim == 1:
        low, high = pieces[3], pieces[4]
        half = low.shape[0]
        index = lax.rem(me + 2, n)
        out[0:half, pl.ds(index, 1)] = low[...][:, None]
        out[half : 2 * half, pl.ds(index, 1)] = high[...][:, None]


def beside(at, slot, pieces, dim):
    dims = list(pieces[0].shape)
    dims.insert(dim, 4)
    return pl.pallas_call(
        functools.partial(beside_kernel, dim, 4, slot),
        out_shape=shape_of(dims),
        in_specs=[SMEM] + [VMEM] * len(pieces),
        out_specs=VMEM,
        name="beside",
    )(at, *pieces)


def ring4(block, axis):
    half = block.shape[0] // 2
    back = shift(block, axis, 1)
    ahead = shift(block, axis, -1)
    low = shift(back[:half], axis, 1)
    high = shift(ahead[half:], axis, -1)
    return block, back, ahead, low, high


def direct4(at, slot, block, axis):
    back = shift(block, axis, 1)
    ahead = shift(block, axis, -1)
    far = shift(block, axis, 2)
    return beside(at, slot, (block, back, ahead, far), 0)


def ring8(block, axis):
    half = block.shape[0] // 2
    back = ahead = block
    pieces = [block]
    for _ in range(3):
        back = shift(back, axis, 1)
        ahead = shift(ahead, axis, -1)
        pieces += [back, ahead]
    return (*pieces, shift(back[:half], axis, 1), shift(ahead[half:], axis, -1))


def attend_kernel(tokens, at, own, other, cos_ref, sin_ref, *refs):
    a_pieces, b_pieces = refs[0:5], refs[5:10]
    ctx, w_a, w_b, normed, q_s, k_s, v_s, sems = refs[10:]
    width = own.shape[1]
    x_at, y_at = at[1], at[2]
    a_copies, b_copies = [], []
    for i, (by, start, size) in enumerate(((0, 0, 1), (3, 0, 1), (1, 0, 1), (2, 0, 2), (2, 1, 2))):
        y_from = lax.rem(y_at + by, 4)
        x_from = lax.rem(x_at + by, 4)
        for j in range(4 // size):
            a_copies.append(
                pltpu.make_async_copy(
                    a_pieces[i].at[j], w_a.at[:, y_from, j + start * 2], sems.at[4 * i + j]
                )
            )
        z = pl.ds(start * 4, 8 // size)
        b_copies.append(pltpu.make_async_copy(b_pieces[i], w_b.at[z, :, x_from], sems.at[20 + i]))
    for c in a_copies:
        c.start()
    n = k_s.shape[1]
    for c in a_copies:
        c.wait()
    for c in b_copies:
        c.start()
    gain = w_a[:, :, :, :, 2 * n : 2 * n + PAD].reshape(width // PAD, PAD, PAD).astype(F32)
    eye = lax.broadcasted_iota(jnp.int32, (PAD, PAD), 0) == lax.broadcasted_iota(jnp.int32, (PAD, PAD), 1)
    lanes = jnp.concatenate(
        [jnp.sum(jnp.where(eye, gain[i], 0.0), axis=0, keepdims=True) for i in range(width // PAD)], axis=1
    )
    step = 32

    def norm(i, _):
        for s, ref in enumerate((own, other)):
            start = pl.multiple_of(i * step, step)
            x = ref[pl.ds(start, step), :].astype(F32)
            inv = lax.rsqrt(jnp.sum(x * x, axis=1, keepdims=True) * (1.0 / width) + norm_eps)
            normed[pl.ds(s * tokens + start, step), :] = (x * inv * lanes).astype(BF16)
        return 0

    lax.fori_loop(0, tokens // step, norm, 0)

    low_half = (lax.broadcasted_iota(jnp.int32, (2 * tokens, 2 * HD), 1) % HD) < HD // 2

    def rope(t):
        turned = jnp.where(low_half, -pltpu.roll(t, 2 * HD - HD // 2, 1), pltpu.roll(t, HD // 2, 1))
        both = lambda ref: jnp.concatenate([ref[...], ref[...]], axis=0)
        return t * both(cos_ref) + turned * both(sin_ref)

    def product(ref, start):
        weights = ref[:, :, :, :, start : start + n].reshape(width, n)
        return jnp.dot(normed[...], weights, preferred_element_type=F32)

    def store(t, to, start):
        for j in range(n // (2 * HD)):
            cols = slice(j * 2 * HD, (j + 1) * 2 * HD)
            to[:, start + j * 2 * HD : start + (j + 1) * 2 * HD] = rope(t[:, cols]).astype(BF16)

    store(product(w_a, 0), k_s, 0)
    v_s[...] = product(w_a, n).astype(BF16)
    store(product(w_a, 2 * n + PAD), q_s, 0)
    for c in b_copies:
        c.wait()
    for k in range(3):
        store(product(w_b, k * n), q_s, (k + 1) * n)

    seen = lax.broadcasted_iota(jnp.int32, (tokens, tokens), 0) >= lax.broadcasted_iota(
        jnp.int32, (tokens, tokens), 1
    )
    left = lax.broadcasted_iota(jnp.int32, (tokens, 2 * HD), 1) < HD

    def softmax(scores):
        scores = jnp.where(seen, scores, -1e30)
        expo = jnp.exp(scores - jnp.max(scores, axis=1, keepdims=True))
        return (expo * (1.0 / jnp.sum(expo, axis=1, keepdims=True))).astype(BF16)

    def attend(s, _):
        rows = pl.ds(pl.multiple_of(s * tokens, tokens), tokens)
        for kv in range(4):

            def sides(ref, scale):
                tile = ref[rows, (kv // 2) * 2 * HD : (kv // 2 + 1) * 2 * HD].astype(F32) * scale
                a = jnp.where(left, tile if kv % 2 == 0 else pltpu.roll(tile, HD, 1), 0.0)
                return jnp.concatenate([a, pltpu.roll(a, HD, 1)], axis=0).astype(BF16)

            pairs = [slice((kv * 2 + p) * 2 * HD, (kv * 2 + p + 1) * 2 * HD) for p in range(2)]
            scores = lax.dot_general(
                jnp.concatenate([q_s[rows, cols] for cols in pairs], axis=0),
                sides(k_s, HD**-0.5),
                (((1,), (1,)), ((), ())),
                preferred_element_type=F32,
            )
            block = lambda i, j: scores[i * tokens : (i + 1) * tokens, j * tokens : (j + 1) * tokens]
            probs = jnp.concatenate(
                [jnp.concatenate([softmax(block(i, j)) for j in range(2)], axis=1) for i in range(2)], axis=0
            )
            out = jnp.dot(probs, sides(v_s, 1.0), preferred_element_type=F32).astype(BF16)
            for p, cols in enumerate(pairs):
                ctx[rows, cols] = out[p * tokens : (p + 1) * tokens]
        return 0

    lax.fori_loop(0, 2, attend, 0)


def project_kernel(seq, tokens, at, ctx, *refs):
    pieces = refs[0:9]
    out, w_o, sems = refs[9:]
    z_at = at[3]
    rows = w_o.shape[1]
    half = rows // 2
    copies = []
    for i, by in enumerate((0, 7, 1, 6, 2, 5, 3, 4, 4)):
        z_from = lax.rem(z_at + by, 8)
        to = w_o.at[z_from]
        if i == 7:
            to = w_o.at[z_from, 0:half]
        if i == 8:
            to = w_o.at[z_from, half:rows]
        copies.append(pltpu.make_async_copy(pieces[i], to, sems.at[i]))
    for c in copies:
        c.start()
    for c in copies:
        c.wait()

    def one(z, _):
        out[:, pl.ds(pl.multiple_of(z * rows, rows), rows)] = lax.dot_general(
            ctx[seq * tokens : (seq + 1) * tokens, :],
            w_o[z],
            (((1,), (1,)), ((), ())),
            preferred_element_type=F32,
        )
        return 0

    lax.fori_loop(0, 8, one, 0)


def inner(hidden, attn_gain, w_query, w_key, w_value, w_out):
    tokens, width = hidden.shape
    wq, wkv = w_query.shape[1] // 2, w_key.shape[1] // 2
    rows = w_query.shape[0]
    cols = wq + 2 * wkv + PAD
    cols_a = 3 * wkv + PAD
    cols_b = cols - cols_a
    at = jnp.stack([lax.axis_index(a) for a in ("c", "x", "y", "z")]).astype(jnp.int32)

    gain = attn_gain[None]
    copies, mine, theirs = pl.pallas_call(
        halves_kernel,
        out_shape=(shape_of((16, rows, cols)), shape_of((rows, wq)), shape_of((rows, wq))),
        in_specs=[SMEM] + [VMEM] * 5,
        out_specs=(VMEM,) * 3,
        name="halves",
    )(at, gain, w_key, w_value, w_query, w_out.T)
    by_z = to_all(copies, ("z", "c")).reshape(8, 2 * rows, cols)
    got = shift(theirs, "c", 1)
    out_rows = pl.pallas_call(
        order_kernel,
        out_shape=shape_of((2 * rows, wq)),
        in_specs=[SMEM, VMEM, VMEM],
        out_specs=VMEM,
        name="order",
    )(at, mine, got)
    other = shift(hidden, "c", 1)
    side_a, side_b = pl.pallas_call(
        split_kernel,
        out_shape=(shape_of((4, 8, 2 * rows, cols_a)), shape_of((8, 2 * rows, cols_b))),
        in_specs=[VMEM],
        out_specs=(VMEM,) * 2,
        name="split",
    )(by_z)
    out_x = direct4(at, 1, out_rows, "x")
    out_xy = direct4(at, 2, out_x, "y").reshape(-1, wq)
    out_pieces = ring8(out_xy, "z")
    block_a = to_all(side_a, "x")
    block_b = beside(at, 2, ring4(side_b, "y"), 1)
    a_pieces = ring4(block_a, "y")
    b_pieces = ring4(block_b, "x")

    position = jnp.arange(tokens, dtype=F32)
    freq = rope_base ** (-(jnp.arange(HD // 2, dtype=F32) * 2.0) / HD)
    angle = position[:, None] * freq[None, :]
    cos_table = jnp.concatenate([jnp.cos(angle)] * 4, axis=-1)
    sin_table = jnp.concatenate([jnp.sin(angle)] * 4, axis=-1)

    context = pl.pallas_call(
        functools.partial(attend_kernel, tokens),
        out_shape=shape_of((2 * tokens, wq)),
        in_specs=[SMEM] + [VMEM] * 4 + [ANY] * 10,
        out_specs=VMEM,
        scratch_shapes=[
            pltpu.VMEM((8, 4, 4, 2 * rows, cols_a), BF16),
            pltpu.VMEM((8, 4, 4, 2 * rows, cols_b), BF16),
            pltpu.VMEM((2 * tokens, width), BF16),
            pltpu.VMEM((2 * tokens, wq), BF16),
            pltpu.VMEM((2 * tokens, wkv), BF16),
            pltpu.VMEM((2 * tokens, wkv), BF16),
            pltpu.SemaphoreType.DMA((25,)),
        ],
        cost_estimate=pl.CostEstimate(
            flops=4_000_000_000, bytes_accessed=10_000_000, transcendentals=0
        ),
        compiler_params=pltpu.CompilerParams(vmem_limit_bytes=40 * 1024 * 1024),
        name="att",
    )(at, hidden, other, cos_table, sin_table, *a_pieces, *b_pieces)

    def project(seq):
        return pl.pallas_call(
            functools.partial(project_kernel, seq, tokens),
            out_shape=shape_of((tokens, width), F32),
            in_specs=[SMEM, VMEM] + [ANY] * 9,
            out_specs=VMEM,
            scratch_shapes=[pltpu.VMEM((8, width // 8, wq), BF16), pltpu.SemaphoreType.DMA((9,))],
            cost_estimate=pl.CostEstimate(flops=1_000_000_000, bytes_accessed=8_000_000, transcendentals=0),
            compiler_params=pltpu.CompilerParams(vmem_limit_bytes=24 * 1024 * 1024),
            name="project",
        )(at, context, *out_pieces)

    from_them = shift(project(1), "c", 1)
    return (hidden.astype(F32) + (project(0) + from_them)).astype(BF16)


def solution(mesh):
    torus = Mesh(mesh.devices.reshape(8, 4, 4, 2), AXES)
    placed = (P(AXES, None), P(AXES), P(AXES, None), P(AXES, None), P(AXES, None), P(None, AXES))
    return jax.shard_map(inner, mesh=torus, in_specs=placed, out_specs=P(AXES, None), check_vma=False)
```

```python
import functools

import jax
import jax.numpy as jnp
from jax import lax
from jax.experimental import pallas as pl
from jax.experimental.pallas import tpu as pltpu
from jax.sharding import Mesh
from jax.sharding import PartitionSpec as P


HD = 64
PAD = 128
AXES = ("z", "y", "x", "c")
VMEM = pl.BlockSpec(memory_space=pltpu.VMEM)
SMEM = pl.BlockSpec(memory_space=pltpu.SMEM)
ANY = pl.BlockSpec(memory_space=pl.ANY)
F32 = jnp.float32
BF16 = jnp.bfloat16

rope_base = 500000.0
norm_eps = 1e-05


def shape_of(dims, dtype=BF16):
    return jax.ShapeDtypeStruct(tuple(dims), dtype)


def shift(array, axis, by):
    n = lax.axis_size(axis)
    return lax.ppermute(array, axis, [(i, (i + by) % n) for i in range(n)])


def halves_kernel(at, gain, wk, wv, wq, wo, copies, mine, theirs):
    core = at[0]
    rows = wq.shape[0]
    eye = lax.broadcasted_iota(jnp.int32, (rows, rows), 0) == lax.broadcasted_iota(jnp.int32, (rows, rows), 1)
    column = jnp.sum(jnp.where(eye, gain[...].astype(F32), 0.0), axis=1, keepdims=True)
    wide = jnp.broadcast_to(column, (rows, PAD)).astype(BF16)
    for which in range(2):
        pieces = []
        for ref in (wk, wv, wq):
            n = ref.shape[1] // 2
            pieces.append(ref[:, which * n : (which + 1) * n])
        row = jnp.concatenate(pieces[:2] + [wide] + pieces[2:], axis=1)
        for z in range(copies.shape[0] // 2):
            copies[2 * z + which] = row
    n = wo.shape[1] // 2
    mine[...] = wo[:, pl.ds(pl.multiple_of(core * n, 128), n)]
    theirs[...] = wo[:, pl.ds(pl.multiple_of((1 - core) * n, 128), n)]


def order_kernel(at, mine, got, out):
    rows = mine.shape[0]
    for k in range(2):
        out[k * rows : (k + 1) * rows, :] = jnp.where(at[0] == k, mine[...], got[...])


def to_all(array, axes):
    return lax.all_to_all(array, axes, split_axis=0, concat_axis=0, tiled=True)


def beside_kernel(dim, n, slot, at, *refs):
    *pieces, out = refs
    me = at[slot]
    for by, ref in zip((0, n - 1, 1, 2, 2), pieces):
        index = lax.rem(me + by, n)
        if dim == 0:
            out[index] = ref[...]
        elif ref.shape[0] == out.shape[0]:
            out[:, pl.ds(index, 1)] = ref[...][:, None]
    if dim == 1:
        low, high = pieces[3], pieces[4]
        half = low.shape[0]
        index = lax.rem(me + 2, n)
        out[0:half, pl.ds(index, 1)] = low[...][:, None]
        out[half : 2 * half, pl.ds(index, 1)] = high[...][:, None]


def beside(at, slot, pieces, dim):
    dims = list(pieces[0].shape)
    dims.insert(dim, 4)
    return pl.pallas_call(
        functools.partial(beside_kernel, dim, 4, slot),
        out_shape=shape_of(dims),
        in_specs=[SMEM] + [VMEM] * len(pieces),
        out_specs=VMEM,
        name="beside",
    )(at, *pieces)


def ring4(block, axis):
    half = block.shape[0] // 2
    back = shift(block, axis, 1)
    ahead = shift(block, axis, -1)
    low = shift(back[:half], axis, 1)
    high = shift(ahead[half:], axis, -1)
    return block, back, ahead, low, high


def direct4(at, slot, block, axis):
    back = shift(block, axis, 1)
    ahead = shift(block, axis, -1)
    far = shift(block, axis, 2)
    return beside(at, slot, (block, back, ahead, far), 0)


def ring8(block, axis):
    half = block.shape[0] // 2
    back = ahead = block
    pieces = [block]
    for _ in range(3):
        back = shift(back, axis, 1)
        ahead = shift(ahead, axis, -1)
        pieces += [back, ahead]
    return (*pieces, shift(back[:half], axis, 1), shift(ahead[half:], axis, -1))


def attend_kernel(tokens, at, own, other, cos_ref, sin_ref, *refs):
    a_pieces, b_pieces = refs[0:5], refs[5:10]
    ctx, w_a, w_b, normed, inv_s, q_s, k_s, v_s, sems = refs[10:]
    width = own.shape[1]
    x_at, y_at = at[1], at[2]
    a_copies, b_copies = [], []
    for i, (by, start, size) in enumerate(((0, 0, 1), (3, 0, 1), (1, 0, 1), (2, 0, 2), (2, 1, 2))):
        y_from = lax.rem(y_at + by, 4)
        x_from = lax.rem(x_at + by, 4)
        for j in range(4 // size):
            a_copies.append(
                pltpu.make_async_copy(
                    a_pieces[i].at[j], w_a.at[:, y_from, j + start * 2], sems.at[4 * i + j]
                )
            )
        z = pl.ds(start * 4, 8 // size)
        b_copies.append(pltpu.make_async_copy(b_pieces[i], w_b.at[z, :, x_from], sems.at[20 + i]))
    for c in a_copies:
        c.start()
    n = k_s.shape[1]
    step = 32

    def inverse(i, _):
        for s, ref in enumerate((own, other)):
            start = pl.multiple_of(i * step, step)
            x = ref[pl.ds(start, step), :].astype(F32)
            inv = lax.rsqrt(jnp.sum(x * x, axis=1, keepdims=True) * (1.0 / width) + norm_eps)
            inv_s[pl.ds(s * tokens + start, step), :] = jnp.broadcast_to(inv, (step, PAD))
        return 0

    lax.fori_loop(0, tokens // step, inverse, 0)
    for c in a_copies:
        c.wait()
    for c in b_copies:
        c.start()
    gain = w_a[:, :, :, :, 2 * n : 2 * n + PAD].reshape(width // PAD, PAD, PAD).astype(F32)
    eye = lax.broadcasted_iota(jnp.int32, (PAD, PAD), 0) == lax.broadcasted_iota(jnp.int32, (PAD, PAD), 1)
    lanes = jnp.concatenate(
        [jnp.sum(jnp.where(eye, gain[i], 0.0), axis=0, keepdims=True) for i in range(width // PAD)], axis=1
    )

    def norm(i, _):
        for s, ref in enumerate((own, other)):
            start = pl.multiple_of(i * step, step)
            to = pl.ds(s * tokens + start, step)
            x = ref[pl.ds(start, step), :].astype(F32)
            normed[to, :] = (x * inv_s[to, 0:1] * lanes).astype(BF16)
        return 0

    lax.fori_loop(0, tokens // step, norm, 0)

    low_half = (lax.broadcasted_iota(jnp.int32, (2 * tokens, 2 * HD), 1) % HD) < HD // 2

    def rope(t):
        turned = jnp.where(low_half, -pltpu.roll(t, 2 * HD - HD // 2, 1), pltpu.roll(t, HD // 2, 1))
        both = lambda ref: jnp.concatenate([ref[...], ref[...]], axis=0)
        return t * both(cos_ref) + turned * both(sin_ref)

    def product(ref, start):
        weights = ref[:, :, :, :, start : start + n].reshape(width, n)
        return jnp.dot(normed[...], weights, preferred_element_type=F32)

    def store(t, to, start):
        for j in range(n // (2 * HD)):
            cols = slice(j * 2 * HD, (j + 1) * 2 * HD)
            to[:, start + j * 2 * HD : start + (j + 1) * 2 * HD] = rope(t[:, cols]).astype(BF16)

    store(product(w_a, 0), k_s, 0)
    v_s[...] = product(w_a, n).astype(BF16)
    store(product(w_a, 2 * n + PAD), q_s, 0)
    for c in b_copies:
        c.wait()
    for k in range(3):
        store(product(w_b, k * n), q_s, (k + 1) * n)

    seen = lax.broadcasted_iota(jnp.int32, (tokens, tokens), 0) >= lax.broadcasted_iota(
        jnp.int32, (tokens, tokens), 1
    )
    left = lax.broadcasted_iota(jnp.int32, (tokens, 2 * HD), 1) < HD

    def softmax(scores):
        scores = jnp.where(seen, scores, -1e30)
        expo = jnp.exp(scores - jnp.max(scores, axis=1, keepdims=True))
        return (expo * (1.0 / jnp.sum(expo, axis=1, keepdims=True))).astype(BF16)

    def attend(s, _):
        rows = pl.ds(pl.multiple_of(s * tokens, tokens), tokens)
        for kv in range(4):

            def sides(ref, scale):
                tile = ref[rows, (kv // 2) * 2 * HD : (kv // 2 + 1) * 2 * HD].astype(F32) * scale
                a = jnp.where(left, tile if kv % 2 == 0 else pltpu.roll(tile, HD, 1), 0.0)
                return jnp.concatenate([a, pltpu.roll(a, HD, 1)], axis=0).astype(BF16)

            pairs = [slice((kv * 2 + p) * 2 * HD, (kv * 2 + p + 1) * 2 * HD) for p in range(2)]
            scores = lax.dot_general(
                jnp.concatenate([q_s[rows, cols] for cols in pairs], axis=0),
                sides(k_s, HD**-0.5),
                (((1,), (1,)), ((), ())),
                preferred_element_type=F32,
            )
            block = lambda i, j: scores[i * tokens : (i + 1) * tokens, j * tokens : (j + 1) * tokens]
            probs = jnp.concatenate(
                [jnp.concatenate([softmax(block(i, j)) for j in range(2)], axis=1) for i in range(2)], axis=0
            )
            out = jnp.dot(probs, sides(v_s, 1.0), preferred_element_type=F32).astype(BF16)
            for p, cols in enumerate(pairs):
                ctx[rows, cols] = out[p * tokens : (p + 1) * tokens]
        return 0

    lax.fori_loop(0, 2, attend, 0)


def project_kernel(seq, tokens, at, ctx, *refs):
    pieces = refs[0:9]
    out, w_o, sems = refs[9:]
    z_at = at[3]
    rows = w_o.shape[1]
    half = rows // 2
    copies = []
    for i, by in enumerate((0, 7, 1, 6, 2, 5, 3, 4, 4)):
        z_from = lax.rem(z_at + by, 8)
        to = w_o.at[z_from]
        if i == 7:
            to = w_o.at[z_from, 0:half]
        if i == 8:
            to = w_o.at[z_from, half:rows]
        copies.append(pltpu.make_async_copy(pieces[i], to, sems.at[i]))
    for c in copies:
        c.start()
    for c in copies:
        c.wait()

    for z in range(8):
        out[:, z * rows : (z + 1) * rows] = lax.dot_general(
            ctx[seq * tokens : (seq + 1) * tokens, :],
            w_o[z],
            (((1,), (1,)), ((), ())),
            preferred_element_type=F32,
        )


def inner(hidden, attn_gain, w_query, w_key, w_value, w_out):
    tokens, width = hidden.shape
    wq, wkv = w_query.shape[1] // 2, w_key.shape[1] // 2
    rows = w_query.shape[0]
    cols = wq + 2 * wkv + PAD
    cols_a = 3 * wkv + PAD
    cols_b = cols - cols_a
    at = jnp.stack([lax.axis_index(a) for a in ("c", "x", "y", "z")]).astype(jnp.int32)

    gain = attn_gain[None]
    copies, mine, theirs = pl.pallas_call(
        halves_kernel,
        out_shape=(shape_of((16, rows, cols)), shape_of((rows, wq)), shape_of((rows, wq))),
        in_specs=[SMEM] + [VMEM] * 5,
        out_specs=(VMEM,) * 3,
        name="halves",
    )(at, gain, w_key, w_value, w_query, w_out.T)
    by_z = to_all(copies, ("z", "c")).reshape(8, 2 * rows, cols)
    got = shift(theirs, "c", 1)
    out_rows = pl.pallas_call(
        order_kernel,
        out_shape=shape_of((2 * rows, wq)),
        in_specs=[SMEM, VMEM, VMEM],
        out_specs=VMEM,
        name="order",
    )(at, mine, got)
    other = shift(hidden, "c", 1)
    side_a = jnp.broadcast_to(by_z[:, :, :cols_a], (4, 8, 2 * rows, cols_a))
    side_b = by_z[:, :, cols_a:]
    out_x = direct4(at, 1, out_rows, "x")
    out_xy = direct4(at, 2, out_x, "y").reshape(-1, wq)
    out_pieces = ring8(out_xy, "z")
    block_a = to_all(side_a, "x")
    block_b = beside(at, 2, ring4(side_b, "y"), 1)
    a_pieces = ring4(block_a, "y")
    b_pieces = ring4(block_b, "x")

    position = jnp.arange(tokens, dtype=F32)
    freq = rope_base ** (-(jnp.arange(HD // 2, dtype=F32) * 2.0) / HD)
    angle = position[:, None] * freq[None, :]
    cos_table = jnp.concatenate([jnp.cos(angle)] * 4, axis=-1)
    sin_table = jnp.concatenate([jnp.sin(angle)] * 4, axis=-1)

    context = pl.pallas_call(
        functools.partial(attend_kernel, tokens),
        out_shape=shape_of((2 * tokens, wq)),
        in_specs=[SMEM] + [VMEM] * 4 + [ANY] * 10,
        out_specs=VMEM,
        scratch_shapes=[
            pltpu.VMEM((8, 4, 4, 2 * rows, cols_a), BF16),
            pltpu.VMEM((8, 4, 4, 2 * rows, cols_b), BF16),
            pltpu.VMEM((2 * tokens, width), BF16),
            pltpu.VMEM((2 * tokens, PAD), F32),
            pltpu.VMEM((2 * tokens, wq), BF16),
            pltpu.VMEM((2 * tokens, wkv), BF16),
            pltpu.VMEM((2 * tokens, wkv), BF16),
            pltpu.SemaphoreType.DMA((25,)),
        ],
        cost_estimate=pl.CostEstimate(
            flops=4_000_000_000, bytes_accessed=10_000_000, transcendentals=0
        ),
        compiler_params=pltpu.CompilerParams(vmem_limit_bytes=40 * 1024 * 1024),
        name="att",
    )(at, hidden, other, cos_table, sin_table, *a_pieces, *b_pieces)

    def project(seq):
        return pl.pallas_call(
            functools.partial(project_kernel, seq, tokens),
            out_shape=shape_of((tokens, width), F32),
            in_specs=[SMEM, VMEM] + [ANY] * 9,
            out_specs=VMEM,
            scratch_shapes=[pltpu.VMEM((8, width // 8, wq), BF16), pltpu.SemaphoreType.DMA((9,))],
            cost_estimate=pl.CostEstimate(flops=1_000_000_000, bytes_accessed=8_000_000, transcendentals=0),
            compiler_params=pltpu.CompilerParams(vmem_limit_bytes=24 * 1024 * 1024),
            name="project",
        )(at, context, *out_pieces)

    from_them = shift(project(1), "c", 1)
    return (hidden.astype(F32) + (project(0) + from_them)).astype(BF16)


def solution(mesh):
    torus = Mesh(mesh.devices.reshape(8, 4, 4, 2), AXES)
    placed = (P(AXES, None), P(AXES), P(AXES, None), P(AXES, None), P(AXES, None), P(None, AXES))
    return jax.shard_map(inner, mesh=torus, in_specs=placed, out_specs=P(AXES, None), check_vma=False)
```

```python
import functools

import jax
import jax.numpy as jnp
from jax import lax
from jax.experimental import pallas as pl
from jax.experimental.pallas import tpu as pltpu
from jax.sharding import Mesh
from jax.sharding import PartitionSpec as P


HD = 64
PAD = 128
AXES = ("z", "y", "x", "c")
VMEM = pl.BlockSpec(memory_space=pltpu.VMEM)
ANY = pl.BlockSpec(memory_space=pl.ANY)
F32 = jnp.float32
BF16 = jnp.bfloat16

rope_base = 500000.0
norm_eps = 1e-05


def position():
    return [lax.axis_index(a) for a in ("c", "x", "y", "z")]


def shape_of(dims, dtype=BF16):
    return jax.ShapeDtypeStruct(tuple(dims), dtype)


def shift(array, axis, by):
    n = lax.axis_size(axis)
    return lax.ppermute(array, axis, [(i, (i + by) % n) for i in range(n)])


def halves_kernel(gain, wk, wv, wq, wo, copies, mine, theirs):
    core = lax.axis_index("c")
    rows = wq.shape[0]
    eye = lax.broadcasted_iota(jnp.int32, (rows, rows), 0) == lax.broadcasted_iota(jnp.int32, (rows, rows), 1)
    column = jnp.sum(jnp.where(eye, gain[...].astype(F32), 0.0), axis=1, keepdims=True)
    wide = jnp.broadcast_to(column, (rows, PAD)).astype(BF16)
    for which in range(2):
        pieces = []
        for ref in (wk, wv, wq):
            n = ref.shape[1] // 2
            pieces.append(ref[:, which * n : (which + 1) * n])
        row = jnp.concatenate(pieces[:2] + [wide] + pieces[2:], axis=1)
        for z in range(copies.shape[0] // 2):
            copies[2 * z + which] = row
    n = wo.shape[1] // 2
    mine[...] = wo[:, pl.ds(pl.multiple_of(core * n, 128), n)]
    theirs[...] = wo[:, pl.ds(pl.multiple_of((1 - core) * n, 128), n)]


def order_kernel(mine, got, out):
    at = position()
    rows = mine.shape[0]
    for k in range(2):
        out[k * rows : (k + 1) * rows, :] = jnp.where(at[0] == k, mine[...], got[...])


def to_all(array, axes):
    return lax.all_to_all(array, axes, split_axis=0, concat_axis=0, tiled=True)


def beside_kernel(dim, n, slot, *refs):
    at = position()
    *pieces, out = refs
    me = at[slot]
    for by, ref in zip((0, n - 1, 1, 2, 2), pieces):
        index = lax.rem(me + by, n)
        if dim == 0:
            out[index] = ref[...]
        elif ref.shape[0] == out.shape[0]:
            out[:, pl.ds(index, 1)] = ref[...][:, None]
    if dim == 1:
        low, high = pieces[3], pieces[4]
        half = low.shape[0]
        index = lax.rem(me + 2, n)
        out[0:half, pl.ds(index, 1)] = low[...][:, None]
        out[half : 2 * half, pl.ds(index, 1)] = high[...][:, None]


def beside(slot, pieces, dim):
    dims = list(pieces[0].shape)
    dims.insert(dim, 4)
    return pl.pallas_call(
        functools.partial(beside_kernel, dim, 4, slot),
        out_shape=shape_of(dims),
        in_specs=[VMEM] * len(pieces),
        out_specs=VMEM,
        name="beside",
    )(*pieces)


def ring4(block, axis):
    half = block.shape[0] // 2
    back = shift(block, axis, 1)
    ahead = shift(block, axis, -1)
    low = shift(back[:half], axis, 1)
    high = shift(ahead[half:], axis, -1)
    return block, back, ahead, low, high


def direct4(slot, block, axis):
    back = shift(block, axis, 1)
    ahead = shift(block, axis, -1)
    far = shift(block, axis, 2)
    return beside(slot, (block, back, ahead, far), 0)


def ring8(block, axis):
    half = block.shape[0] // 2
    back = ahead = block
    pieces = [block]
    for _ in range(3):
        back = shift(back, axis, 1)
        ahead = shift(ahead, axis, -1)
        pieces += [back, ahead]
    return (*pieces, shift(back[:half], axis, 1), shift(ahead[half:], axis, -1))


def attend_kernel(tokens, own, other, cos_ref, sin_ref, *refs):
    a_pieces, b_pieces = refs[0:5], refs[5:10]
    ctx, w_a, w_b, normed, inv_s, q_s, k_s, v_s, sems = refs[10:]
    width = own.shape[1]
    at = position()
    x_at, y_at = at[1], at[2]
    a_copies, b_copies = [], []
    for i, (by, start, size) in enumerate(((0, 0, 1), (3, 0, 1), (1, 0, 1), (2, 0, 2), (2, 1, 2))):
        y_from = lax.rem(y_at + by, 4)
        x_from = lax.rem(x_at + by, 4)
        for j in range(4 // size):
            a_copies.append(
                pltpu.make_async_copy(
                    a_pieces[i].at[j], w_a.at[:, y_from, j + start * 2], sems.at[4 * i + j]
                )
            )
        z = pl.ds(start * 4, 8 // size)
        b_copies.append(pltpu.make_async_copy(b_pieces[i], w_b.at[z, :, x_from], sems.at[20 + i]))
    for c in a_copies:
        c.start()
    n = k_s.shape[1]
    step = 32

    def inverse(i, _):
        for s, ref in enumerate((own, other)):
            start = pl.multiple_of(i * step, step)
            x = ref[pl.ds(start, step), :].astype(F32)
            inv = lax.rsqrt(jnp.sum(x * x, axis=1, keepdims=True) * (1.0 / width) + norm_eps)
            inv_s[pl.ds(s * tokens + start, step), :] = jnp.broadcast_to(inv, (step, PAD))
        return 0

    lax.fori_loop(0, tokens // step, inverse, 0)
    for c in a_copies:
        c.wait()
    for c in b_copies:
        c.start()
    gain = w_a[:, :, :, :, 2 * n : 2 * n + PAD].reshape(width // PAD, PAD, PAD).astype(F32)
    eye = lax.broadcasted_iota(jnp.int32, (PAD, PAD), 0) == lax.broadcasted_iota(jnp.int32, (PAD, PAD), 1)
    lanes = jnp.concatenate(
        [jnp.sum(jnp.where(eye, gain[i], 0.0), axis=0, keepdims=True) for i in range(width // PAD)], axis=1
    )

    def norm(i, _):
        for s, ref in enumerate((own, other)):
            start = pl.multiple_of(i * step, step)
            to = pl.ds(s * tokens + start, step)
            x = ref[pl.ds(start, step), :].astype(F32)
            normed[to, :] = (x * inv_s[to, 0:1] * lanes).astype(BF16)
        return 0

    lax.fori_loop(0, tokens // step, norm, 0)

    low_half = (lax.broadcasted_iota(jnp.int32, (2 * tokens, 2 * HD), 1) % HD) < HD // 2

    def rope(t):
        turned = jnp.where(low_half, -pltpu.roll(t, 2 * HD - HD // 2, 1), pltpu.roll(t, HD // 2, 1))
        both = lambda ref: jnp.concatenate([ref[...], ref[...]], axis=0)
        return t * both(cos_ref) + turned * both(sin_ref)

    def product(ref, start):
        weights = ref[:, :, :, :, start : start + n].reshape(width, n)
        return jnp.dot(normed[...], weights, preferred_element_type=F32)

    def store(t, to, start):
        for j in range(n // (2 * HD)):
            cols = slice(j * 2 * HD, (j + 1) * 2 * HD)
            to[:, start + j * 2 * HD : start + (j + 1) * 2 * HD] = rope(t[:, cols]).astype(BF16)

    store(product(w_a, 0), k_s, 0)
    v_s[...] = product(w_a, n).astype(BF16)
    store(product(w_a, 2 * n + PAD), q_s, 0)
    for c in b_copies:
        c.wait()
    for k in range(3):
        store(product(w_b, k * n), q_s, (k + 1) * n)

    seen = lax.broadcasted_iota(jnp.int32, (tokens, tokens), 0) >= lax.broadcasted_iota(
        jnp.int32, (tokens, tokens), 1
    )
    left = lax.broadcasted_iota(jnp.int32, (tokens, 2 * HD), 1) < HD

    def softmax(scores):
        scores = jnp.where(seen, scores, -1e30)
        expo = jnp.exp(scores - jnp.max(scores, axis=1, keepdims=True))
        return (expo * (1.0 / jnp.sum(expo, axis=1, keepdims=True))).astype(BF16)

    def attend(s, _):
        rows = pl.ds(pl.multiple_of(s * tokens, tokens), tokens)
        for kv in range(4):

            def sides(ref, scale):
                tile = ref[rows, (kv // 2) * 2 * HD : (kv // 2 + 1) * 2 * HD].astype(F32) * scale
                a = jnp.where(left, tile if kv % 2 == 0 else pltpu.roll(tile, HD, 1), 0.0)
                return jnp.concatenate([a, pltpu.roll(a, HD, 1)], axis=0).astype(BF16)

            pairs = [slice((kv * 2 + p) * 2 * HD, (kv * 2 + p + 1) * 2 * HD) for p in range(2)]
            scores = lax.dot_general(
                jnp.concatenate([q_s[rows, cols] for cols in pairs], axis=0),
                sides(k_s, HD**-0.5),
                (((1,), (1,)), ((), ())),
                preferred_element_type=F32,
            )
            block = lambda i, j: scores[i * tokens : (i + 1) * tokens, j * tokens : (j + 1) * tokens]
            probs = jnp.concatenate(
                [jnp.concatenate([softmax(block(i, j)) for j in range(2)], axis=1) for i in range(2)], axis=0
            )
            out = jnp.dot(probs, sides(v_s, 1.0), preferred_element_type=F32).astype(BF16)
            for p, cols in enumerate(pairs):
                ctx[rows, cols] = out[p * tokens : (p + 1) * tokens]
        return 0

    lax.fori_loop(0, 2, attend, 0)


def project_kernel(seq, tokens, ctx, *refs):
    pieces = refs[0:9]
    out, w_o, sems = refs[9:]
    z_at = position()[3]
    rows = w_o.shape[1]
    half = rows // 2
    copies = []
    for i, by in enumerate((0, 7, 1, 6, 2, 5, 3, 4, 4)):
        z_from = lax.rem(z_at + by, 8)
        to = w_o.at[z_from]
        if i == 7:
            to = w_o.at[z_from, 0:half]
        if i == 8:
            to = w_o.at[z_from, half:rows]
        copies.append(pltpu.make_async_copy(pieces[i], to, sems.at[i]))
    for c in copies:
        c.start()
    for c in copies:
        c.wait()

    for z in range(8):
        out[:, z * rows : (z + 1) * rows] = lax.dot_general(
            ctx[seq * tokens : (seq + 1) * tokens, :],
            w_o[z],
            (((1,), (1,)), ((), ())),
            preferred_element_type=F32,
        )


def inner(hidden, attn_gain, w_query, w_key, w_value, w_out):
    tokens, width = hidden.shape
    wq, wkv = w_query.shape[1] // 2, w_key.shape[1] // 2
    rows = w_query.shape[0]
    cols = wq + 2 * wkv + PAD
    cols_a = 3 * wkv + PAD
    cols_b = cols - cols_a

    gain = attn_gain[None]
    copies, mine, theirs = pl.pallas_call(
        halves_kernel,
        out_shape=(shape_of((16, rows, cols)), shape_of((rows, wq)), shape_of((rows, wq))),
        in_specs=[VMEM] * 5,
        out_specs=(VMEM,) * 3,
        name="halves",
    )(gain, w_key, w_value, w_query, w_out.T)
    by_z = to_all(copies, ("z", "c")).reshape(8, 2 * rows, cols)
    got = shift(theirs, "c", 1)
    out_rows = pl.pallas_call(
        order_kernel,
        out_shape=shape_of((2 * rows, wq)),
        in_specs=[VMEM, VMEM],
        out_specs=VMEM,
        name="order",
    )(mine, got)
    other = shift(hidden, "c", 1)
    side_a = jnp.broadcast_to(by_z[:, :, :cols_a], (4, 8, 2 * rows, cols_a))
    side_b = by_z[:, :, cols_a:]
    out_x = direct4(1, out_rows, "x")
    out_xy = direct4(2, out_x, "y").reshape(-1, wq)
    out_pieces = ring8(out_xy, "z")
    block_a = to_all(side_a, "x")
    block_b = beside(2, ring4(side_b, "y"), 1)
    a_pieces = ring4(block_a, "y")
    b_pieces = ring4(block_b, "x")

    position = jnp.arange(tokens, dtype=F32)
    freq = rope_base ** (-(jnp.arange(HD // 2, dtype=F32) * 2.0) / HD)
    angle = position[:, None] * freq[None, :]
    cos_table = jnp.concatenate([jnp.cos(angle)] * 4, axis=-1)
    sin_table = jnp.concatenate([jnp.sin(angle)] * 4, axis=-1)

    context = pl.pallas_call(
        functools.partial(attend_kernel, tokens),
        out_shape=shape_of((2 * tokens, wq)),
        in_specs=[VMEM] * 4 + [ANY] * 10,
        out_specs=VMEM,
        scratch_shapes=[
            pltpu.VMEM((8, 4, 4, 2 * rows, cols_a), BF16),
            pltpu.VMEM((8, 4, 4, 2 * rows, cols_b), BF16),
            pltpu.VMEM((2 * tokens, width), BF16),
            pltpu.VMEM((2 * tokens, PAD), F32),
            pltpu.VMEM((2 * tokens, wq), BF16),
            pltpu.VMEM((2 * tokens, wkv), BF16),
            pltpu.VMEM((2 * tokens, wkv), BF16),
            pltpu.SemaphoreType.DMA((25,)),
        ],
        cost_estimate=pl.CostEstimate(
            flops=4_000_000_000, bytes_accessed=10_000_000, transcendentals=0
        ),
        compiler_params=pltpu.CompilerParams(vmem_limit_bytes=40 * 1024 * 1024),
        name="att",
    )(hidden, other, cos_table, sin_table, *a_pieces, *b_pieces)

    def project(seq):
        return pl.pallas_call(
            functools.partial(project_kernel, seq, tokens),
            out_shape=shape_of((tokens, width), F32),
            in_specs=[VMEM] + [ANY] * 9,
            out_specs=VMEM,
            scratch_shapes=[pltpu.VMEM((8, width // 8, wq), BF16), pltpu.SemaphoreType.DMA((9,))],
            cost_estimate=pl.CostEstimate(flops=1_000_000_000, bytes_accessed=8_000_000, transcendentals=0),
            compiler_params=pltpu.CompilerParams(vmem_limit_bytes=24 * 1024 * 1024),
            name="project",
        )(context, *out_pieces)

    from_them = shift(project(1), "c", 1)
    return (hidden.astype(F32) + (project(0) + from_them)).astype(BF16)


def solution(mesh):
    torus = Mesh(mesh.devices.reshape(8, 4, 4, 2), AXES)
    placed = (P(AXES, None), P(AXES), P(AXES, None), P(AXES, None), P(AXES, None), P(None, AXES))
    return jax.shard_map(inner, mesh=torus, in_specs=placed, out_specs=P(AXES, None), check_vma=False)
```
